32 devices in a mesh: gx: 8 (over z, x), gy: 4 (over y, core).
Axes of the slice: x: 2, y: 2, z: 4, core: 2. Of those that a mesh axis runs over, the one named last changes fastest.
Arguments:
- right_side: float32 [3, 224, 12432], P(None, 'gx', 'gy'), may hold values from -6 to 6
- guess: float32 [3, 224, 12432], P(None, 'gx', 'gy'), may hold values from -6 to 6
- material: int32 [32, 16, 16], P('gx', 'gy'), may hold values from 0 to 7
- lame: float32 [2, 8], replicated, may hold values from 0.5 to 2
- upper: float32 [1], replicated, may hold values from 3 to 6
- lower_ratio: float32 [1], replicated, may hold values from 0.05 to 0.3
Outputs:
- smoothed: float32 [3, 224, 12432], P(None, 'gx', 'gy')
- residual: float32 [3, 224, 12432], P(None, 'gx', 'gy')
The draws below stay inside these ranges and needn't reach their ends.
All inputs are finite; a program needn't handle non-finite values.
Results may differ from the reference program's by a relative error of at most 0.0003.
Values sent between devices are 32-bit elements; how exact they have to be, the bound alone decides.
A program may use at most 128 MiB of HBM per device.

```python
import math
import jax
import jax.numpy as jnp
import numpy as np
from jax import lax

DEG = 7
EZ = 16
NMAT = 8
SWEEPS = 2
CHEB = 3
NEX = 32
NEY = 16
NXN = 224
NYN = 112
ZN = 111


def plant(entries, rng, smallest, largest):
    dims = entries.shape
    place = [jax.random.randint(jax.random.fold_in(rng, axis), (), 0, dims[axis]) for axis in range(len(dims))]
    entries = entries.at[tuple(place)].set(smallest)
    longest = dims.index(max(dims))
    place[longest] = (place[longest] + 1) % dims[longest]
    return entries.at[tuple(place)].set(largest)


def block_levels(own_key, dims, split, low, largest):
    loudness = 1.0
    for axis_at, parts in split:
        heights = jax.random.uniform(jax.random.fold_in(jax.random.fold_in(own_key, 6), axis_at), (parts,), jnp.float32, low / len(split), largest / len(split))
        loudness = loudness * jnp.repeat(jnp.exp(heights), dims[axis_at] // parts).reshape((-1,) + (1,) * (len(dims) - 1 - axis_at))
    return loudness


def normal_values(own_key, shape, spread, most, cuts=(), kind=jnp.bfloat16):
    drawn = spread * jax.random.normal(own_key, shape, jnp.float32)
    if cuts:
        drawn = drawn * block_levels(own_key, shape, cuts, -0.22, 0.18)
    return jnp.clip(drawn, -most, most).astype(kind)


def setup_inputs(seed: int = 0) -> dict:
    seeds = jax.random.split(jax.random.key(seed), 7)
    return {
        "right_side": normal_values(seeds[0], (3, NXN, NYN * ZN), 0.5, 6.0, ((1, 8), (2, 4)), jnp.float32),
        "guess": normal_values(seeds[1], (3, NXN, NYN * ZN), 1.0, 6.0, ((1, 8), (2, 4)), jnp.float32),
        "material": plant(jax.random.randint(seeds[2], (NEX, NEY, EZ), 0, NMAT), jax.random.fold_in(seeds[2], 1), 0, NMAT - 1).astype(jnp.int32),
        "lame": jnp.clip(jnp.exp(jax.random.uniform(seeds[3], (2, NMAT), jnp.float32, math.log(0.5), math.log(2.0))), 0.5, 2.0),
        "upper": jnp.clip(jax.random.uniform(seeds[4], (1,), jnp.float32, 3.0, 6.0), 3.0, 6.0),
        "lower_ratio": jnp.clip(jax.random.uniform(seeds[5], (1,), jnp.float32, 0.05, 0.3), 0.05, 0.3),
    }


highest = lax.Precision.HIGHEST


def legendre_pair(points, degree):
    prev_poly = points * 0.0 + 1.0
    this_poly = points * 1.0
    for order in range(2, degree + 1):
        next_poly = ((2 * order - 1) * points * this_poly - (order - 1) * prev_poly) / order
        prev_poly = this_poly
        this_poly = next_poly
    return this_poly, prev_poly


def gll_tables(degree):
    count = degree + 1
    points = -np.cos(np.pi * np.arange(count) / degree)
    for newton_step in range(60):
        this_poly, prev_poly = legendre_pair(points, degree)
        points = points - (points * this_poly - prev_poly) / (count * this_poly)
    values, unused_poly = legendre_pair(points, degree)
    weights = 2.0 / (degree * (degree + 1) * values ** 2)
    identity_np = np.eye(count)
    spacing = points[:, None] - points[None, :] + identity_np
    derivative = values[:, None] / (values[None, :] * spacing) * (1.0 - identity_np)
    derivative[0, 0] = -degree * (degree + 1) / 4.0
    derivative[degree, degree] = degree * (degree + 1) / 4.0
    stiff_ratio = (weights[:, None] * derivative ** 2).sum(0) / weights
    return weights, derivative, stiff_ratio


def split_periodic(field_in, dim_index):
    layout = field_in.shape
    blocks = layout[dim_index] // DEG
    leading = field_in.reshape(layout[:dim_index] + (blocks, DEG) + layout[dim_index + 1:])
    first_node = lax.slice_in_dim(leading, 0, 1, axis=dim_index + 1)
    return jnp.concatenate([leading, jnp.roll(first_node, -1, axis=dim_index)], axis=dim_index + 1)


def fold_periodic(element_vals, dim_index):
    layout = element_vals.shape
    blocks = layout[dim_index]
    leading = lax.slice_in_dim(element_vals, 0, DEG, axis=dim_index + 1)
    trailing = lax.slice_in_dim(element_vals, DEG, DEG + 1, axis=dim_index + 1)
    first_node = lax.slice_in_dim(leading, 0, 1, axis=dim_index + 1) + jnp.roll(trailing, 1, axis=dim_index)
    remaining = lax.slice_in_dim(leading, 1, DEG, axis=dim_index + 1)
    joined = jnp.concatenate([first_node, remaining], axis=dim_index + 1)
    return joined.reshape(layout[:dim_index] + (blocks * DEG,) + layout[dim_index + 2:])


def split_clamped(field_in):
    layout = field_in.shape
    blocks = (layout[-1] + 1) // DEG
    widths = [(0, 0)] * (len(layout) - 1) + [(1, 1)]
    padded = jnp.pad(field_in, widths)
    leading = padded[..., :blocks * DEG].reshape(layout[:-1] + (blocks, DEG))
    trailing = padded[..., DEG::DEG][..., None]
    joined = jnp.concatenate([leading, trailing], -1)
    return joined.reshape(layout[:-1] + (blocks * (DEG + 1),))


def fold_clamped(element_vals):
    layout = element_vals.shape
    blocks = layout[-1] // (DEG + 1)
    split_vals = element_vals.reshape(layout[:-1] + (blocks, DEG + 1))
    leading = split_vals[..., :DEG].reshape(layout[:-1] + (blocks * DEG,))
    trailing = split_vals[..., DEG:]
    filler = jnp.zeros(layout[:-1] + (blocks, DEG - 1), element_vals.dtype)
    spread_tail = jnp.concatenate([filler, trailing], -1).reshape(layout[:-1] + (blocks * DEG,))
    no_pad = [(0, 0)] * (len(layout) - 1)
    full_line = jnp.pad(leading, no_pad + [(0, 1)]) + jnp.pad(spread_tail, no_pad + [(1, 0)])
    return full_line[..., 1:blocks * DEG]


def along_z(field_in, matrix):
    layout = field_in.shape
    split_vals = field_in.reshape(layout[:-1] + (layout[-1] // (DEG + 1), DEG + 1))
    return jnp.einsum('pk,...k->...p', matrix, split_vals, precision=highest).reshape(layout)


def element_forces(element_vals, lam_w, mu_w, derivative, z_grad, z_back):
    grad_x = jnp.einsum('pi,cxiyjz->cxpyjz', derivative, element_vals, precision=highest)
    grad_y = jnp.einsum('pj,cxiyjz->cxiypz', derivative, element_vals, precision=highest)
    grad_z = along_z(element_vals, z_grad)
    gradients = jnp.stack([grad_x, grad_y, grad_z])
    divergence = gradients[0, 0] + gradients[1, 1] + gradients[2, 2]
    identity = jnp.eye(3, dtype=jnp.float32).reshape(3, 3, 1, 1, 1, 1, 1)
    stress = mu_w * (gradients + jnp.swapaxes(gradients, 0, 1)) + lam_w * divergence * identity
    forces = jnp.einsum('pi,cxpyjz->cxiyjz', derivative, stress[0], precision=highest)
    forces = forces + jnp.einsum('pj,cxiypz->cxiyjz', derivative, stress[1], precision=highest)
    return forces + along_z(stress[2], z_back)


def element_diagonal(lam_w, mu_w, ratio_x, ratio_y, ratio_z):
    ratio_sum = ratio_x + ratio_y + ratio_z
    pieces = [lam_w * own_ratio + mu_w * (ratio_sum + own_ratio) for own_ratio in (ratio_x, ratio_y, ratio_z)]
    return jnp.stack(pieces)


def point_weight(weights, blocks_z):
    weights_z = jnp.tile(weights, blocks_z)
    return weights[None, :, None, None, None] * weights[None, None, None, :, None] * weights_z[None, None, None, None, :]


def point_coeffs(lam_el, mu_el, point_w):
    lam_rep = jnp.repeat(lam_el, DEG + 1, axis=2)[:, None, :, None, :]
    mu_rep = jnp.repeat(mu_el, DEG + 1, axis=2)[:, None, :, None, :]
    return lam_rep * point_w, mu_rep * point_w


def lame_fields(material, lame):
    labels = jnp.arange(lame.shape[1], dtype=jnp.int32)
    onehot = (material[..., None] == labels).astype(jnp.float32)
    coeffs = jnp.einsum('xyzm,km->kxyz', onehot, lame, precision=highest)
    return coeffs[0], coeffs[1]


def assemble_slabs(results):
    return fold_clamped(fold_periodic(jnp.moveaxis(results, 0, 1), 1))


def reference(right_side, guess, material, lame, upper, lower_ratio):
    weights_np, derivative_np, ratio_np = gll_tables(DEG)
    weights = jnp.asarray(weights_np, dtype=jnp.float32)
    derivative = jnp.asarray(derivative_np, dtype=jnp.float32)
    stiff_ratio = jnp.asarray(ratio_np, dtype=jnp.float32)
    point_w = point_weight(weights, EZ)
    ratio_x = stiff_ratio.reshape(1, DEG + 1, 1, 1, 1)
    ratio_y = stiff_ratio.reshape(1, 1, 1, DEG + 1, 1)
    ratio_z = jnp.tile(stiff_ratio, EZ).reshape(1, 1, 1, 1, -1)
    lam_el, mu_el = lame_fields(material, lame)
    shape_four = (3, NXN, NYN, ZN)
    source = right_side.reshape(shape_four)
    solution = guess.reshape(shape_four)

    def operate(field_in):
        slabs = jnp.moveaxis(split_periodic(split_clamped(field_in), 1), 1, 0)

        def one_slab(inputs):
            column_slab, lam_slab, mu_slab = inputs
            lam_w, mu_w = point_coeffs(lam_slab[None], mu_slab[None], point_w)
            element_vals = split_periodic(column_slab, 2)[:, None]
            forces = element_forces(element_vals, lam_w, mu_w, derivative, derivative, derivative.T)
            return fold_periodic(forces[:, 0], 2)

        return assemble_slabs(lax.map(one_slab, (slabs, lam_el, mu_el)))

    def diag_slab(inputs):
        lam_slab, mu_slab = inputs
        lam_w, mu_w = point_coeffs(lam_slab[None], mu_slab[None], point_w)
        pieces = element_diagonal(lam_w, mu_w, ratio_x, ratio_y, ratio_z)
        return fold_periodic(pieces[:, 0], 2)

    diagonal = assemble_slabs(lax.map(diag_slab, (lam_el, mu_el)))
    inverse = 1.0 / diagonal
    upper_edge = upper[0]
    lower_edge = lower_ratio[0] * upper_edge
    center = (upper_edge + lower_edge) / 2.0
    radius = (upper_edge - lower_edge) / 2.0
    sigma_ratio = center / radius
    for sweep_index in range(SWEEPS):
        residual = source - operate(solution)
        change = inverse * residual / center
        solution = solution + change
        factor = 1.0 / sigma_ratio
        for step_index in range(CHEB - 1):
            factor_next = 1.0 / (2.0 * sigma_ratio - factor)
            residual = source - operate(solution)
            change = factor_next * factor * change + (2.0 * factor_next / radius) * inverse * residual
            solution = solution + change
            factor = factor_next
    residual = source - operate(solution)
    flat_shape = (3, NXN, NYN * ZN)
    return solution.reshape(flat_shape), residual.reshape(flat_shape)
```

```python
import jax
import jax.numpy as jnp
import numpy as np
from jax import lax
from jax.experimental import pallas as pl
from jax.experimental.pallas import tpu as pltpu
from jax.sharding import PartitionSpec as P

DEG = 7
SWEEPS = 2
CHEB = 3


highest = lax.Precision.HIGHEST


def legendre_pair(points, degree):
    prev_poly = points * 0.0 + 1.0
    this_poly = points * 1.0
    for order in range(2, degree + 1):
        next_poly = ((2 * order - 1) * points * this_poly - (order - 1) * prev_poly) / order
        prev_poly = this_poly
        this_poly = next_poly
    return (this_poly, prev_poly)


def gll_tables(degree):
    count = degree + 1
    points = -np.cos(np.pi * np.arange(count) / degree)
    for newton_step in range(60):
        this_poly, prev_poly = legendre_pair(points, degree)
        points = points - (points * this_poly - prev_poly) / (count * this_poly)
    values, unused_poly = legendre_pair(points, degree)
    weights = 2.0 / (degree * (degree + 1) * values**2)
    identity_np = np.eye(count)
    spacing = points[:, None] - points[None, :] + identity_np
    derivative = values[:, None] / (values[None, :] * spacing) * (1.0 - identity_np)
    derivative[0, 0] = -degree * (degree + 1) / 4.0
    derivative[degree, degree] = degree * (degree + 1) / 4.0
    stiff_ratio = (weights[:, None] * derivative**2).sum(0) / weights
    return (weights, derivative, stiff_ratio)


def clamped_gather(blocks):
    free_nodes = DEG * blocks - 1
    selector = np.zeros((free_nodes, blocks * (DEG + 1)), np.float32)
    for element in range(blocks):
        for node_idx in range(DEG + 1):
            target = DEG * element + node_idx - 1
            if 0 <= target < free_nodes:
                selector[target, element * (DEG + 1) + node_idx] = 1.0
    return selector


def lame_fields(material, lame):
    labels = jnp.arange(lame.shape[1], dtype=jnp.int32)
    onehot = (material[..., None] == labels).astype(jnp.float32)
    coeffs = jnp.einsum("xyzm,km->kxyz", onehot, lame, precision=highest)
    return (coeffs[0], coeffs[1])


N1 = DEG + 1
SLOTS = 4


def halves(value):
    high = value.astype(jnp.bfloat16)
    low = (value - high.astype(jnp.float32)).astype(jnp.bfloat16)
    return high, low


def np_halves(matrix):
    high = np.asarray(matrix, np.float32).astype(jnp.bfloat16)
    low = (np.asarray(matrix, np.float64) - high.astype(np.float64)).astype(jnp.bfloat16)
    return high, low


def apply_pairs(matrix, values):
    half = N1 // 2
    even = [values[i] + values[DEG - i] for i in range(half)]
    odd = [values[i] - values[DEG - i] for i in range(half)]
    outs = [None] * N1
    for p in range(half):
        plus = None
        minus = None
        for i in range(half):
            by_even = float(np.float32((matrix[p, i] + matrix[p, DEG - i]) / 2))
            by_odd = float(np.float32((matrix[p, i] - matrix[p, DEG - i]) / 2))
            plus = by_even * even[i] if plus is None else plus + by_even * even[i]
            minus = by_odd * odd[i] if minus is None else minus + by_odd * odd[i]
        outs[p] = minus + plus
        outs[DEG - p] = minus - plus
    return outs


def smoother_kernel(
    steps,
    elems_x,
    elems_y,
    derivative,
    coef,
    guess,
    source,
    lam_in,
    mu_in,
    weight_in,
    own_in,
    sum_in,
    grad_in,
    back_in,
    join_in,
    field,
    resid,
    lam_w,
    mu_w,
    inverse,
    change,
    grad_x,
    grad_y,
    grad_z,
    send_x,
    send_y,
    send_c,
    recv_x,
    recv_y,
    recv_c,
    send_sem,
    recv_sem,
):
    cols = elems_x * elems_y
    size_x = lax.axis_size("gx")
    size_y = lax.axis_size("gy")
    me_x = lax.axis_index("gx")
    me_y = lax.axis_index("gy")
    near_x = (lax.rem(me_x + size_x - 1, size_x), lax.rem(me_x + 1, size_x))
    near_y = (lax.rem(me_y + size_y - 1, size_y), lax.rem(me_y + 1, size_y))
    partners = [(near_x[0], me_y), (near_x[1], me_y), (me_x, near_y[0]), (me_x, near_y[1])]
    partners += [(near_x[a], near_y[b]) for a in range(2) for b in range(2)]

    barrier = pltpu.get_barrier_semaphore()
    for partner in partners:
        pl.semaphore_signal(
            barrier, inc=1, device_id=partner, device_id_type=pl.DeviceIdType.MESH
        )
    pl.semaphore_wait(barrier, len(partners))

    def copies(slot):
        made = []
        for d in range(8):
            if d < 2:
                src, dst = send_x.at[slot, d], recv_x.at[slot, 1 - d]
            elif d < 4:
                src, dst = send_y.at[slot, d - 2], recv_y.at[slot, 3 - d]
            else:
                src, dst = send_c.at[slot, d - 4], recv_c.at[slot, 7 - d]
            mirror = (1, 0, 3, 2, 7, 6, 5, 4)[d]
            made.append(
                pltpu.make_async_remote_copy(
                    src_ref=src,
                    dst_ref=dst,
                    send_sem=send_sem.at[slot, d],
                    recv_sem=recv_sem.at[slot, mirror],
                    device_id=partners[d],
                    device_id_type=pl.DeviceIdType.MESH,
                )
            )
        return made

    rows = lax.broadcasted_iota(jnp.int32, (N1 * cols, 128), 0) % cols
    row_y = rows % elems_y
    inner_low_x = rows >= elems_y
    inner_high_x = rows < cols - elems_y
    inner_low_y = row_y >= 1
    inner_high_y = row_y < elems_y - 1

    def local_sum(ref):
        flat = (N1 * cols, 128)
        full = (N1, cols, 128)
        zero = jnp.zeros(flat, jnp.float32)
        for c in range(3):
            low = ref[c, 0].reshape(flat)
            high = ref[c, DEG].reshape(flat)
            to_low = jnp.where(inner_low_x, pltpu.roll(high, elems_y, 0), zero)
            to_high = jnp.where(inner_high_x, pltpu.roll(low, N1 * cols - elems_y, 0), zero)
            ref[c, 0] = (low + to_low).reshape(full)
            ref[c, DEG] = (high + to_high).reshape(full)
        for c in range(3):
            low = ref[c, :, 0].reshape(flat)
            high = ref[c, :, DEG].reshape(flat)
            to_low = jnp.where(inner_low_y, pltpu.roll(high, 1, 0), zero)
            to_high = jnp.where(inner_high_y, pltpu.roll(low, N1 * cols - 1, 0), zero)
            ref[c, :, 0] = (low + to_low).reshape(full)
            ref[c, :, DEG] = (high + to_high).reshape(full)

    last_x = cols - elems_y
    last_y = elems_y - 1

    def post(ref, slot):
        for c in range(3):
            send_x[slot, 0, c] = ref[c, 0, :, 0:elems_y, :]
            send_x[slot, 1, c] = ref[c, DEG, :, last_x:cols, :]
            for a in range(elems_x):
                send_y[slot, 0, c, :, a : a + 1, :] = ref[c, :, 0, a * elems_y : a * elems_y + 1, :]
                at = a * elems_y + last_y
                send_y[slot, 1, c, :, a : a + 1, :] = ref[c, :, DEG, at : at + 1, :]
            for a in range(2):
                for b in range(2):
                    at = a * last_x + b * last_y
                    send_c[slot, 2 * a + b, c] = ref[c, a * DEG, b * DEG, at : at + 1, :]
        for copy in copies(slot):
            copy.start()

    def collect(ref, slot):
        for copy in copies(slot):
            copy.wait()
        for c in range(3):
            ref[c, 0, :, 0:elems_y, :] += recv_x[slot, 0, c]
            ref[c, DEG, :, last_x:cols, :] += recv_x[slot, 1, c]
            for a in range(elems_x):
                at = a * elems_y
                ref[c, :, 0, at : at + 1, :] += recv_y[slot, 0, c, :, a : a + 1, :]
                at = a * elems_y + last_y
                ref[c, :, DEG, at : at + 1, :] += recv_y[slot, 1, c, :, a : a + 1, :]
            for a in range(2):
                for b in range(2):
                    at = a * last_x + b * last_y
                    ref[c, a * DEG, b * DEG, at : at + 1, :] += recv_c[slot, 2 * a + b, c]

    @pl.loop(0, 3 * N1)
    def _(at):
        c = at // N1
        i = at % N1
        field[c, i] = guess[c, i]

    local_sum(field)
    post(field, 0)

    lam_all = lam_in[...]
    mu_all = mu_in[...]

    @pl.loop(0, N1)
    def _(i):
        for j in range(N1):
            lam_w[i, j] = lam_all * weight_in[i, j]
            mu_w[i, j] = mu_all * weight_in[i, j]

    @pl.loop(0, 3 * N1)
    def _(at):
        c = at // N1
        i = at % N1
        pieces = []
        for j in range(N1):
            own = own_in[c, i, j]
            pieces.append(lam_w[i, j] * own + mu_w[i, j] * (sum_in[i, j] + own))
        high, low = halves(jnp.concatenate(pieces, axis=0))
        summed = jnp.dot(
            jnp.concatenate([high, low], axis=1), join_in[...], preferred_element_type=jnp.float32
        )
        inverse[c, i] = summed.reshape(N1, cols, 128)

    local_sum(inverse)
    post(inverse, 1)
    collect(field, 0)
    collect(inverse, 1)

    @pl.loop(0, 3 * N1)
    def _(at):
        c = at // N1
        i = at % N1
        inverse[c, i] = 1.0 / inverse[c, i]
        change[c, i] = jnp.zeros((N1, cols, 128), jnp.float32)

    def operator():
        @pl.loop(0, 3 * N1)
        def _(at):
            c = at // N1
            j = at % N1
            for p, out in enumerate(apply_pairs(derivative, [field[c, i, j] for i in range(N1)])):
                grad_x[c, p, j] = out

        @pl.loop(0, 3 * N1)
        def _(at):
            c = at // N1
            i = at % N1
            for q, out in enumerate(apply_pairs(derivative, [field[c, i, j] for j in range(N1)])):
                grad_y[c, i, q] = out

        @pl.loop(0, 3 * N1 // 2)
        def _(at):
            c = at // (N1 // 2)
            i = at % (N1 // 2)
            high, low = halves(field[c, pl.ds(2 * i, 2)].reshape(2 * N1 * cols, 128))
            both = jnp.dot(
                jnp.concatenate([high, low], axis=1),
                grad_in[...],
                preferred_element_type=jnp.float32,
            )
            grad_z[c, pl.ds(2 * i, 2)] = (both[:, :128] + both[:, 128:]).reshape(2, N1, cols, 128)

        @pl.loop(0, N1)
        def _(i):
            for j in range(N1):
                lam = lam_w[i, j]
                mu = mu_w[i, j]
                d00, d11, d22 = grad_x[0, i, j], grad_y[1, i, j], grad_z[2, i, j]
                base = lam * (d00 + d11 + d22)
                two = mu + mu
                grad_x[0, i, j] = two * d00 + base
                grad_y[1, i, j] = two * d11 + base
                grad_z[2, i, j] = two * d22 + base
                s01 = mu * (grad_x[1, i, j] + grad_y[0, i, j])
                s02 = mu * (grad_x[2, i, j] + grad_z[0, i, j])
                s12 = mu * (grad_y[2, i, j] + grad_z[1, i, j])
                grad_x[1, i, j] = s01
                grad_y[0, i, j] = s01
                grad_x[2, i, j] = s02
                grad_z[0, i, j] = s02
                grad_y[2, i, j] = s12
                grad_z[1, i, j] = s12

        @pl.loop(0, 3 * N1)
        def _(at):
            c = at // N1
            j = at % N1
            for p, out in enumerate(apply_pairs(derivative.T, [grad_x[c, i, j] for i in range(N1)])):
                resid[c, p, j] = out

        @pl.loop(0, 3 * N1)
        def _(at):
            c = at // N1
            i = at % N1
            for q, out in enumerate(apply_pairs(derivative.T, [grad_y[c, i, j] for j in range(N1)])):
                resid[c, i, q] += out

        @pl.loop(0, 3 * N1 // 2)
        def _(at):
            c = at // (N1 // 2)
            i = at % (N1 // 2)
            pick = pl.ds(2 * i, 2)
            parts = halves(resid[c, pick].reshape(2 * N1 * cols, 128))
            parts += halves(grad_z[c, pick].reshape(2 * N1 * cols, 128))
            both = jnp.dot(
                jnp.concatenate(parts, axis=1), back_in[...], preferred_element_type=jnp.float32
            )
            force = (both[:, :128] + both[:, 128:]).reshape(2, N1, cols, 128)
            resid[c, pick] = source[c, pick] - force

    @pl.loop(0, steps + 1)
    def _(step):
        operator()
        local_sum(resid)
        slot = 2 + step % 2
        post(resid, slot)
        collect(resid, slot)

        @pl.when(step < steps)
        def _():
            alpha = coef[0, step]
            beta = coef[1, step]

            @pl.loop(0, 3 * N1)
            def _(at):
                c = at // N1
                i = at % N1
                new = alpha * change[c, i] + beta * (inverse[c, i] * resid[c, i])
                change[c, i] = new
                field[c, i] += new


def z_join(blocks, clamped):
    nodes = DEG * blocks + 1
    gather = np.zeros((nodes, blocks * N1))
    for element in range(blocks):
        for k in range(N1):
            gather[DEG * element + k, element * N1 + k] = 1.0
    if clamped:
        gather[0] = 0.0
        gather[nodes - 1] = 0.0
    return gather.T @ gather


def local(right_side, guess, material, lame, upper, lower_ratio):
    elems_x, elems_y, elems_z = material.shape
    cols = elems_x * elems_y
    lanes = N1 * elems_z
    nodes_z = DEG * elems_z - 1
    weights_np, derivative_np, ratio_np = gll_tables(DEG)
    eye_z = np.eye(elems_z)
    grad_np = np.kron(eye_z, derivative_np.T)
    join_np = z_join(elems_z, True)
    back_np = np.kron(eye_z, derivative_np) @ join_np
    grad_high, grad_low = np_halves(grad_np)
    back_high, back_low = np_halves(back_np)
    none = np.zeros_like(grad_high)
    joined = join_np.astype(jnp.bfloat16)
    grad_in = jnp.asarray(np.block([[grad_high, grad_low], [grad_high, none]]))
    back_in = jnp.asarray(
        np.block([[joined, none], [joined, none], [back_high, back_low], [back_high, none]])
    )
    all_join = z_join(elems_z, False).astype(jnp.bfloat16)
    join_in = jnp.asarray(np.concatenate([all_join, all_join], axis=0))

    weights_z = np.tile(weights_np, elems_z)
    ratio_z = np.tile(ratio_np, elems_z)
    weight_np = weights_np[:, None, None] * weights_np[None, :, None] * weights_z
    shape_w = (N1, N1, lanes)
    own_x = np.broadcast_to(ratio_np[:, None, None], shape_w)
    own_y = np.broadcast_to(ratio_np[None, :, None], shape_w)
    own_z = np.broadcast_to(ratio_z, shape_w)
    own_np = np.stack([own_x, own_y, own_z])
    weight_in = jnp.asarray(weight_np[:, :, None], jnp.float32)
    own_in = jnp.asarray(own_np[:, :, :, None], jnp.float32)
    sum_in = jnp.asarray((own_x + own_y + own_z)[:, :, None], jnp.float32)

    lam_el, mu_el = lame_fields(material, lame)
    lam_in = jnp.repeat(lam_el.reshape(cols, elems_z), N1, axis=1)
    mu_in = jnp.repeat(mu_el.reshape(cols, elems_z), N1, axis=1)

    upper_edge = upper[0]
    lower_edge = lower_ratio[0] * upper_edge
    center = (upper_edge + lower_edge) / 2.0
    radius = (upper_edge - lower_edge) / 2.0
    sigma_ratio = center / radius
    alphas = []
    betas = []
    for sweep_index in range(SWEEPS):
        alphas.append(jnp.float32(0.0))
        betas.append(1.0 / center)
        factor = 1.0 / sigma_ratio
        for step_index in range(CHEB - 1):
            factor_next = 1.0 / (2.0 * sigma_ratio - factor)
            alphas.append(factor_next * factor)
            betas.append(2.0 * factor_next / radius)
            factor = factor_next
    coef = jnp.stack([jnp.stack(alphas), jnp.stack(betas)])

    gather_z = jnp.asarray(clamped_gather(elems_z), dtype=jnp.float32)
    owned = clamped_gather(elems_z)
    owned[:, DEG::N1] = 0.0
    select_z = jnp.asarray(owned.T, dtype=jnp.float32)

    def enter(flat):
        split = flat.reshape(3, elems_x, DEG, elems_y, DEG, nodes_z)
        wide = jnp.matmul(split, gather_z, precision=highest)
        wide = wide.transpose(0, 2, 4, 1, 3, 5).reshape(3, DEG, DEG, cols, lanes)
        return jnp.pad(wide, ((0, 0), (0, 1), (0, 1), (0, 0), (0, 0)))

    def leave(wide):
        split = wide[:, :DEG, :DEG].reshape(3, DEG, DEG, elems_x, elems_y, lanes)
        split = split.transpose(0, 3, 1, 4, 2, 5)
        thin = jnp.matmul(split, select_z, precision=highest)
        return thin.reshape(3, DEG * elems_x, DEG * elems_y * nodes_z)

    whole = (3, N1, N1, cols, lanes)
    shape = jax.ShapeDtypeStruct(whole, jnp.float32)
    vmem = pl.BlockSpec(memory_space=pltpu.VMEM)
    big = pltpu.VMEM(whole, jnp.float32)
    small = pltpu.VMEM((N1, N1, cols, lanes), jnp.float32)
    face_x = pltpu.VMEM((SLOTS, 2, 3, N1, elems_y, lanes), jnp.float32)
    face_y = pltpu.VMEM((SLOTS, 2, 3, N1, elems_x, lanes), jnp.float32)
    corner = pltpu.VMEM((SLOTS, 4, 3, 1, lanes), jnp.float32)

    def kernel(*refs):
        smoother_kernel(SWEEPS * CHEB, elems_x, elems_y, derivative_np, *refs)

    field, resid = pl.pallas_call(
        kernel,
        out_shape=(shape, shape),
        in_specs=[pl.BlockSpec(memory_space=pltpu.SMEM)] + [vmem] * 10,
        out_specs=(vmem, vmem),
        scratch_shapes=[
            small,
            small,
            big,
            big,
            big,
            big,
            big,
            face_x,
            face_y,
            corner,
            face_x,
            face_y,
            corner,
            pltpu.SemaphoreType.DMA((SLOTS, 8)),
            pltpu.SemaphoreType.DMA((SLOTS, 8)),
        ],
        compiler_params=pltpu.CompilerParams(collective_id=0, has_side_effects=True),
    )(
        coef,
        enter(guess),
        enter(right_side),
        lam_in,
        mu_in,
        weight_in,
        own_in,
        sum_in,
        grad_in,
        back_in,
        join_in,
    )
    return (leave(field), leave(resid))


def solution(mesh):
    placed = (P(None, "gx", "gy"), P(None, "gx", "gy"), P("gx", "gy", None), P(), P(), P())
    return jax.shard_map(
        local,
        mesh=mesh,
        in_specs=placed,
        out_specs=(P(None, "gx", "gy"), P(None, "gx", "gy")),
        check_vma=False,
    )
```

```python
import jax
import jax.numpy as jnp
import numpy as np
from jax import lax
from jax.experimental import pallas as pl
from jax.experimental.pallas import tpu as pltpu
from jax.sharding import PartitionSpec as P

DEG = 7
SWEEPS = 2
CHEB = 3


highest = lax.Precision.HIGHEST


def legendre_pair(points, degree):
    prev_poly = points * 0.0 + 1.0
    this_poly = points * 1.0
    for order in range(2, degree + 1):
        next_poly = ((2 * order - 1) * points * this_poly - (order - 1) * prev_poly) / order
        prev_poly = this_poly
        this_poly = next_poly
    return (this_poly, prev_poly)


def gll_tables(degree):
    count = degree + 1
    points = -np.cos(np.pi * np.arange(count) / degree)
    for newton_step in range(60):
        this_poly, prev_poly = legendre_pair(points, degree)
        points = points - (points * this_poly - prev_poly) / (count * this_poly)
    values, unused_poly = legendre_pair(points, degree)
    weights = 2.0 / (degree * (degree + 1) * values**2)
    identity_np = np.eye(count)
    spacing = points[:, None] - points[None, :] + identity_np
    derivative = values[:, None] / (values[None, :] * spacing) * (1.0 - identity_np)
    derivative[0, 0] = -degree * (degree + 1) / 4.0
    derivative[degree, degree] = degree * (degree + 1) / 4.0
    stiff_ratio = (weights[:, None] * derivative**2).sum(0) / weights
    return (weights, derivative, stiff_ratio)


def clamped_gather(blocks):
    free_nodes = DEG * blocks - 1
    selector = np.zeros((free_nodes, blocks * (DEG + 1)), np.float32)
    for element in range(blocks):
        for node_idx in range(DEG + 1):
            target = DEG * element + node_idx - 1
            if 0 <= target < free_nodes:
                selector[target, element * (DEG + 1) + node_idx] = 1.0
    return selector


N1 = DEG + 1
SLOTS = 4


def halves(value):
    high = value.astype(jnp.bfloat16)
    low = (value - high.astype(jnp.float32)).astype(jnp.bfloat16)
    return high, low


def np_halves(matrix):
    high = np.asarray(matrix, np.float32).astype(jnp.bfloat16)
    low = (np.asarray(matrix, np.float64) - high.astype(np.float64)).astype(jnp.bfloat16)
    return high, low


def apply_pairs(matrix, values):
    half = N1 // 2
    even = [values[i] + values[DEG - i] for i in range(half)]
    odd = [values[i] - values[DEG - i] for i in range(half)]
    outs = [None] * N1
    for p in range(half):
        plus = None
        minus = None
        for i in range(half):
            by_even = float(np.float32((matrix[p, i] + matrix[p, DEG - i]) / 2))
            by_odd = float(np.float32((matrix[p, i] - matrix[p, DEG - i]) / 2))
            plus = by_even * even[i] if plus is None else plus + by_even * even[i]
            minus = by_odd * odd[i] if minus is None else minus + by_odd * odd[i]
        outs[p] = minus + plus
        outs[DEG - p] = minus - plus
    return outs


def smoother_kernel(
    steps,
    elems_x,
    elems_y,
    derivative,
    lame,
    upper,
    lower_ratio,
    guess_in,
    source_in,
    material,
    weight_in,
    own_in,
    sum_in,
    spread_in,
    gather_in,
    select_in,
    grad_in,
    back_in,
    join_in,
    smoothed_out,
    residual_out,
    coef,
    field,
    resid,
    source,
    lam_w,
    mu_w,
    inverse,
    change,
    grad_x,
    grad_y,
    grad_z,
    flat_a,
    flat_b,
    send_x,
    send_y,
    send_c,
    recv_x,
    recv_y,
    recv_c,
    send_sem,
    recv_sem,
):
    cols = elems_x * elems_y
    size_x = lax.axis_size("gx")
    size_y = lax.axis_size("gy")
    me_x = lax.axis_index("gx")
    me_y = lax.axis_index("gy")
    near_x = (lax.rem(me_x + size_x - 1, size_x), lax.rem(me_x + 1, size_x))
    near_y = (lax.rem(me_y + size_y - 1, size_y), lax.rem(me_y + 1, size_y))
    partners = [(near_x[0], me_y), (near_x[1], me_y), (me_x, near_y[0]), (me_x, near_y[1])]
    partners += [(near_x[a], near_y[b]) for a in range(2) for b in range(2)]

    barrier = pltpu.get_barrier_semaphore()
    for partner in partners:
        pl.semaphore_signal(
            barrier, inc=1, device_id=partner, device_id_type=pl.DeviceIdType.MESH
        )
    pl.semaphore_wait(barrier, len(partners))

    def copies(slot, c):
        made = []
        for d in range(8):
            if d < 2:
                src, dst = send_x.at[slot, c, d], recv_x.at[slot, c, 1 - d]
            elif d < 4:
                src, dst = send_y.at[slot, c, d - 2], recv_y.at[slot, c, 3 - d]
            else:
                src, dst = send_c.at[slot, c, d - 4], recv_c.at[slot, c, 7 - d]
            mirror = (1, 0, 3, 2, 7, 6, 5, 4)[d]
            made.append(
                pltpu.make_async_remote_copy(
                    src_ref=src,
                    dst_ref=dst,
                    send_sem=send_sem.at[slot, c, d],
                    recv_sem=recv_sem.at[slot, c, mirror],
                    device_id=partners[d],
                    device_id_type=pl.DeviceIdType.MESH,
                )
            )
        return made

    rows = lax.broadcasted_iota(jnp.int32, (N1 * cols, 128), 0) % cols
    row_x = rows % elems_x
    inner_low_y = rows >= elems_x
    inner_high_y = rows < cols - elems_x
    inner_low_x = row_x >= 1
    inner_high_x = row_x < elems_x - 1
    last_x = elems_x - 1
    last_y = cols - elems_x
    flat = (N1 * cols, 128)
    full = (N1, cols, 128)

    def local_sum(ref, c):
        zero = jnp.zeros(flat, jnp.float32)
        low = ref[c, 0].reshape(flat)
        high = ref[c, DEG].reshape(flat)
        to_low = jnp.where(inner_low_x, pltpu.roll(high, 1, 0), zero)
        to_high = jnp.where(inner_high_x, pltpu.roll(low, N1 * cols - 1, 0), zero)
        ref[c, 0] = (low + to_low).reshape(full)
        ref[c, DEG] = (high + to_high).reshape(full)
        low = ref[c, :, 0].reshape(flat)
        high = ref[c, :, DEG].reshape(flat)
        to_low = jnp.where(inner_low_y, pltpu.roll(high, elems_x, 0), zero)
        to_high = jnp.where(inner_high_y, pltpu.roll(low, N1 * cols - elems_x, 0), zero)
        ref[c, :, 0] = (low + to_low).reshape(full)
        ref[c, :, DEG] = (high + to_high).reshape(full)

    def post(ref, slot, c):
        send_y[slot, c, 0] = ref[c, :, 0, 0:elems_x, :]
        send_y[slot, c, 1] = ref[c, :, DEG, last_y:cols, :]
        for b in range(elems_y):
            at = b * elems_x
            send_x[slot, c, 0, :, b : b + 1, :] = ref[c, 0, :, at : at + 1, :]
            at = b * elems_x + last_x
            send_x[slot, c, 1, :, b : b + 1, :] = ref[c, DEG, :, at : at + 1, :]
        for a in range(2):
            for b in range(2):
                at = a * last_x + b * last_y
                send_c[slot, c, 2 * a + b] = ref[c, a * DEG, b * DEG, at : at + 1, :]
        for copy in copies(slot, c):
            copy.start()

    def collect(ref, slot, c):
        for copy in copies(slot, c):
            copy.wait()
        ref[c, :, 0, 0:elems_x, :] += recv_y[slot, c, 0]
        ref[c, :, DEG, last_y:cols, :] += recv_y[slot, c, 1]
        for b in range(elems_y):
            at = b * elems_x
            ref[c, 0, :, at : at + 1, :] += recv_x[slot, c, 0, :, b : b + 1, :]
            at = b * elems_x + last_x
            ref[c, DEG, :, at : at + 1, :] += recv_x[slot, c, 1, :, b : b + 1, :]
        for a in range(2):
            for b in range(2):
                at = a * last_x + b * last_y
                ref[c, a * DEG, b * DEG, at : at + 1, :] += recv_c[slot, c, 2 * a + b]

    nodes_x = DEG * elems_x
    nodes_y = DEG * elems_y
    nodes_z = guess_in.shape[2] // nodes_y
    pad_x = flat_a.shape[1]
    zeros_big = jnp.zeros((N1, cols, 128), jnp.float32)

    @pl.loop(0, nodes_y)
    def _(y):
        flat_a[y] = jnp.zeros((pad_x, 128), jnp.float32)
        flat_b[y] = jnp.zeros((pad_x, 128), jnp.float32)

    def through(src, dst, matrix):
        @pl.loop(0, elems_y)
        def _(b):
            pick = pl.ds(b * DEG, DEG)
            parts = halves(src[pick].reshape(DEG * pad_x, 128))
            dst[pick] = jnp.dot(
                jnp.concatenate(parts, axis=1), matrix[...], preferred_element_type=jnp.float32
            ).reshape(DEG, pad_x, 128)

    def enter(flat_in, ref, c):
        lines = flat_in[c]
        for y in range(nodes_y):
            flat_a[y, 0:nodes_x, 0:nodes_z] = lines[:, y * nodes_z : (y + 1) * nodes_z]
        through(flat_a, flat_b, gather_in)
        ref[c, DEG] = zeros_big
        ref[c, :, DEG] = zeros_big
        for b in range(elems_y):
            for j in range(DEG):
                for i in range(DEG):
                    ref[c, i, j, b * elems_x : (b + 1) * elems_x, :] = flat_b[
                        b * DEG + j, pl.ds(i, elems_x, stride=DEG), :
                    ]

    def leave(ref, flat_out, c):
        for b in range(elems_y):
            for j in range(DEG):
                for i in range(DEG):
                    flat_b[b * DEG + j, pl.ds(i, elems_x, stride=DEG), :] = ref[
                        c, i, j, b * elems_x : (b + 1) * elems_x, :
                    ]
        through(flat_b, flat_a, select_in)
        lines = [flat_a[y, 0:nodes_x, 0:nodes_z] for y in range(nodes_y)]
        flat_out[c] = jnp.concatenate(lines, axis=1)

    @pl.loop(0, 3)
    def _(c):
        enter(guess_in, field, c)
        local_sum(field, c)
        post(field, 0, c)

    upper_edge = jnp.full((1, 128), upper[0], jnp.float32)
    lower_edge = lower_ratio[0] * upper_edge
    center = (upper_edge + lower_edge) / 2.0
    radius = (upper_edge - lower_edge) / 2.0
    sigma_ratio = center / radius
    for sweep in range(SWEEPS):
        coef[0, sweep * CHEB] = jnp.zeros((1, 128), jnp.float32)
        coef[1, sweep * CHEB] = 1.0 / center
        factor = 1.0 / sigma_ratio
        for later in range(1, CHEB):
            factor_next = 1.0 / (2.0 * sigma_ratio - factor)
            coef[0, sweep * CHEB + later] = factor_next * factor
            coef[1, sweep * CHEB + later] = 2.0 * factor_next / radius
            factor = factor_next

    kinds = jnp.concatenate([material[:, b, :] for b in range(elems_y)], axis=0)
    tables = []
    for row in range(2):
        picked = jnp.zeros(kinds.shape, jnp.float32)
        for kind in range(lame.shape[1]):
            picked = jnp.where(kinds == kind, lame[row, kind], picked)
        tables.append(
            jnp.dot(picked, spread_in[...], precision=highest, preferred_element_type=jnp.float32)
        )
    lam_all, mu_all = tables

    @pl.loop(0, N1)
    def _(i):
        for j in range(N1):
            lam_w[i, j] = lam_all * weight_in[i, j]
            mu_w[i, j] = mu_all * weight_in[i, j]

    @pl.loop(0, 3 * N1)
    def _(at):
        c = at // N1
        i = at % N1
        pieces = []
        for j in range(N1):
            own = own_in[c, i, j]
            pieces.append(lam_w[i, j] * own + mu_w[i, j] * (sum_in[i, j] + own))
        high, low = halves(jnp.concatenate(pieces, axis=0))
        summed = jnp.dot(
            jnp.concatenate([high, low], axis=1), join_in[...], preferred_element_type=jnp.float32
        )
        inverse[c, i] = summed.reshape(N1, cols, 128)

    for c in range(3):
        local_sum(inverse, c)
        post(inverse, 1, c)

    def gradients(c):
        @pl.loop(0, N1)
        def _(i):
            high, low = halves(field[c, i].reshape(flat))
            both = jnp.dot(
                jnp.concatenate([high, low], axis=1),
                grad_in[...],
                preferred_element_type=jnp.float32,
            )
            for p, out in enumerate(apply_pairs(derivative, [field[c, k, i] for k in range(N1)])):
                grad_x[c, p, i] = out
            for q, out in enumerate(apply_pairs(derivative, [field[c, i, k] for k in range(N1)])):
                grad_y[c, i, q] = out
            grad_z[c, i] = (both[:, :128] + both[:, 128:]).reshape(full)

    def stresses():
        @pl.loop(0, N1)
        def _(i):
            for j in range(N1):
                lam = lam_w[i, j]
                mu = mu_w[i, j]
                d00, d11, d22 = grad_x[0, i, j], grad_y[1, i, j], grad_z[2, i, j]
                base = lam * (d00 + d11 + d22)
                two = mu + mu
                grad_x[0, i, j] = two * d00 + base
                grad_y[1, i, j] = two * d11 + base
                grad_z[2, i, j] = two * d22 + base
                s01 = mu * (grad_x[1, i, j] + grad_y[0, i, j])
                s02 = mu * (grad_x[2, i, j] + grad_z[0, i, j])
                s12 = mu * (grad_y[2, i, j] + grad_z[1, i, j])
                grad_x[1, i, j] = s01
                grad_y[0, i, j] = s01
                grad_x[2, i, j] = s02
                grad_z[0, i, j] = s02
                grad_y[2, i, j] = s12
                grad_z[1, i, j] = s12

    def forces(c):
        @pl.loop(0, N1)
        def _(j):
            for p, out in enumerate(apply_pairs(derivative.T, [grad_x[c, k, j] for k in range(N1)])):
                resid[c, p, j] = out

        @pl.loop(0, N1)
        def _(i):
            outs = apply_pairs(derivative.T, [grad_y[c, i, k] for k in range(N1)])
            inner = jnp.concatenate([resid[c, i, q] + outs[q] for q in range(N1)], axis=0)
            parts = halves(grad_z[c, i].reshape(flat)) + halves(inner)
            both = jnp.dot(
                jnp.concatenate(parts, axis=1), back_in[...], preferred_element_type=jnp.float32
            )
            resid[c, i] = source[c, i] - (both[:, :128] + both[:, 128:]).reshape(full)

    def residuals(slot):
        stresses()

        @pl.loop(0, 3)
        def _(c):
            forces(c)
            local_sum(resid, c)
            post(resid, slot, c)

    @pl.loop(0, 3)
    def _(c):
        enter(source_in, source, c)

    @pl.loop(0, 3)
    def _(c):
        collect(field, 0, c)
        gradients(c)

    @pl.loop(0, 3)
    def _(c):
        collect(inverse, 1, c)

        @pl.loop(0, N1)
        def _(i):
            inverse[c, i] = 1.0 / inverse[c, i]
            change[c, i] = zeros_big

    @pl.loop(0, steps)
    def _(step):
        slot = 2 + step % 2
        residuals(slot)

        @pl.loop(0, 3)
        def _(c):
            collect(resid, slot, c)
            alpha = coef[0, step]
            beta = coef[1, step]

            @pl.loop(0, N1)
            def _(i):
                new = alpha * change[c, i] + beta * (inverse[c, i] * resid[c, i])
                change[c, i] = new
                field[c, i] += new

            gradients(c)

    slot = 2 + steps % 2
    residuals(slot)

    @pl.loop(0, 3)
    def _(c):
        leave(field, smoothed_out, c)

    @pl.loop(0, 3)
    def _(c):
        collect(resid, slot, c)
        leave(resid, residual_out, c)


def z_join(blocks, clamped):
    nodes = DEG * blocks + 1
    gather = np.zeros((nodes, blocks * N1))
    for element in range(blocks):
        for k in range(N1):
            gather[DEG * element + k, element * N1 + k] = 1.0
    if clamped:
        gather[0] = 0.0
        gather[nodes - 1] = 0.0
    return gather.T @ gather


def local(right_side, guess, material, lame, upper, lower_ratio):
    elems_x, elems_y, elems_z = material.shape
    cols = elems_x * elems_y
    lanes = N1 * elems_z
    nodes_z = DEG * elems_z - 1
    weights_np, derivative_np, ratio_np = gll_tables(DEG)
    eye_z = np.eye(elems_z)
    grad_np = np.kron(eye_z, derivative_np.T)
    join_np = z_join(elems_z, True)
    back_np = np.kron(eye_z, derivative_np) @ join_np
    grad_high, grad_low = np_halves(grad_np)
    back_high, back_low = np_halves(back_np)
    none = np.zeros_like(grad_high)
    joined = join_np.astype(jnp.bfloat16)
    grad_in = jnp.asarray(np.block([[grad_high, grad_low], [grad_high, none]]))
    back_in = jnp.asarray(
        np.block([[back_high, back_low], [back_high, none], [joined, none], [joined, none]])
    )
    all_join = z_join(elems_z, False).astype(jnp.bfloat16)
    join_in = jnp.asarray(np.concatenate([all_join, all_join], axis=0))

    weights_z = np.tile(weights_np, elems_z)
    ratio_z = np.tile(ratio_np, elems_z)
    weight_np = weights_np[:, None, None] * weights_np[None, :, None] * weights_z
    shape_w = (N1, N1, lanes)
    own_x = np.broadcast_to(ratio_np[:, None, None], shape_w)
    own_y = np.broadcast_to(ratio_np[None, :, None], shape_w)
    own_z = np.broadcast_to(ratio_z, shape_w)
    own_np = np.stack([own_x, own_y, own_z])
    weight_in = jnp.asarray(weight_np[:, :, None], jnp.float32)
    own_in = jnp.asarray(own_np[:, :, :, None], jnp.float32)
    sum_in = jnp.asarray((own_x + own_y + own_z)[:, :, None], jnp.float32)

    gather_np = clamped_gather(elems_z)
    nodes_z = gather_np.shape[0]
    owned_np = gather_np.copy()
    owned_np[:, DEG::N1] = 0.0
    enter_np = np.zeros((lanes, lanes))
    enter_np[:nodes_z] = gather_np
    leave_np = np.zeros((lanes, lanes))
    leave_np[:, :nodes_z] = owned_np.T
    gather_in = jnp.asarray(np.concatenate([enter_np, enter_np], axis=0).astype(jnp.bfloat16))
    select_in = jnp.asarray(np.concatenate([leave_np, leave_np], axis=0).astype(jnp.bfloat16))
    spread_in = jnp.asarray(np.kron(eye_z, np.ones((1, N1))), dtype=jnp.float32)

    pad_x = -(-DEG * elems_x // 8) * 8
    whole = (3, N1, N1, cols, lanes)
    vmem = pl.BlockSpec(memory_space=pltpu.VMEM)
    smem = pl.BlockSpec(memory_space=pltpu.SMEM)
    big = pltpu.VMEM(whole, jnp.float32)
    small = pltpu.VMEM((N1, N1, cols, lanes), jnp.float32)
    lines = pltpu.VMEM((DEG * elems_y, pad_x, lanes), jnp.float32)
    face_x = pltpu.VMEM((SLOTS, 3, 2, N1, elems_y, lanes), jnp.float32)
    face_y = pltpu.VMEM((SLOTS, 3, 2, N1, elems_x, lanes), jnp.float32)
    corner = pltpu.VMEM((SLOTS, 3, 4, 1, lanes), jnp.float32)
    shape = jax.ShapeDtypeStruct(guess.shape, jnp.float32)

    def kernel(*refs):
        smoother_kernel(SWEEPS * CHEB, elems_x, elems_y, derivative_np, *refs)

    return pl.pallas_call(
        kernel,
        out_shape=(shape, shape),
        in_specs=[smem] * 3 + [vmem] * 12,
        out_specs=(vmem, vmem),
        scratch_shapes=[pltpu.VMEM((2, SWEEPS * CHEB, 1, lanes), jnp.float32)]
        + [big] * 3
        + [small] * 2
        + [big] * 5
        + [lines] * 2
        + [face_x, face_y, corner] * 2
        + [pltpu.SemaphoreType.DMA((SLOTS, 3, 8))] * 2,
        compiler_params=pltpu.CompilerParams(collective_id=0, has_side_effects=True),
    )(
        lame,
        upper,
        lower_ratio,
        guess,
        right_side,
        material,
        weight_in,
        own_in,
        sum_in,
        spread_in,
        gather_in,
        select_in,
        grad_in,
        back_in,
        join_in,
    )


def solution(mesh):
    placed = (P(None, "gx", "gy"), P(None, "gx", "gy"), P("gx", "gy", None), P(), P(), P())
    return jax.shard_map(
        local,
        mesh=mesh,
        in_specs=placed,
        out_specs=(P(None, "gx", "gy"), P(None, "gx", "gy")),
        check_vma=False,
    )
```

```python
import jax
import jax.numpy as jnp
import numpy as np
from jax import lax
from jax.experimental import pallas as pl
from jax.experimental.pallas import tpu as pltpu
from jax.sharding import PartitionSpec as P

DEG = 7
SWEEPS = 2
CHEB = 3


highest = lax.Precision.HIGHEST


def legendre_pair(points, degree):
    prev_poly = points * 0.0 + 1.0
    this_poly = points * 1.0
    for order in range(2, degree + 1):
        next_poly = ((2 * order - 1) * points * this_poly - (order - 1) * prev_poly) / order
        prev_poly = this_poly
        this_poly = next_poly
    return (this_poly, prev_poly)


def gll_tables(degree):
    count = degree + 1
    points = -np.cos(np.pi * np.arange(count) / degree)
    for newton_step in range(60):
        this_poly, prev_poly = legendre_pair(points, degree)
        points = points - (points * this_poly - prev_poly) / (count * this_poly)
    values, unused_poly = legendre_pair(points, degree)
    weights = 2.0 / (degree * (degree + 1) * values**2)
    identity_np = np.eye(count)
    spacing = points[:, None] - points[None, :] + identity_np
    derivative = values[:, None] / (values[None, :] * spacing) * (1.0 - identity_np)
    derivative[0, 0] = -degree * (degree + 1) / 4.0
    derivative[degree, degree] = degree * (degree + 1) / 4.0
    stiff_ratio = (weights[:, None] * derivative**2).sum(0) / weights
    return (weights, derivative, stiff_ratio)


def clamped_gather(blocks):
    free_nodes = DEG * blocks - 1
    selector = np.zeros((free_nodes, blocks * (DEG + 1)), np.float32)
    for element in range(blocks):
        for node_idx in range(DEG + 1):
            target = DEG * element + node_idx - 1
            if 0 <= target < free_nodes:
                selector[target, element * (DEG + 1) + node_idx] = 1.0
    return selector


N1 = DEG + 1
SLOTS = 4


def halves(value):
    high = value.astype(jnp.bfloat16)
    low = (value - high.astype(jnp.float32)).astype(jnp.bfloat16)
    return high, low


def np_halves(matrix):
    high = np.asarray(matrix, np.float32).astype(jnp.bfloat16)
    low = (np.asarray(matrix, np.float64) - high.astype(np.float64)).astype(jnp.bfloat16)
    return high, low


def apply_pairs(matrix, values):
    half = N1 // 2
    even = [values[i] + values[DEG - i] for i in range(half)]
    odd = [values[i] - values[DEG - i] for i in range(half)]
    outs = [None] * N1
    for p in range(half):
        plus = None
        minus = None
        for i in range(half):
            by_even = float(np.float32((matrix[p, i] + matrix[p, DEG - i]) / 2))
            by_odd = float(np.float32((matrix[p, i] - matrix[p, DEG - i]) / 2))
            plus = by_even * even[i] if plus is None else plus + by_even * even[i]
            minus = by_odd * odd[i] if minus is None else minus + by_odd * odd[i]
        outs[p] = minus + plus
        outs[DEG - p] = minus - plus
    return outs


def smoother_kernel(
    steps,
    elems_x,
    elems_y,
    derivative,
    lame,
    upper,
    lower_ratio,
    guess_in,
    source_in,
    material,
    weight_in,
    own_in,
    sum_in,
    spread_in,
    gather_in,
    select_in,
    grad_in,
    back_in,
    join_in,
    smoothed_out,
    residual_out,
    coef,
    field,
    resid,
    source,
    lam_w,
    mu_w,
    inverse,
    change,
    grad_x,
    grad_y,
    grad_z,
    flat_a,
    flat_b,
    send_x,
    send_y,
    send_c,
    recv_x,
    recv_y,
    recv_c,
    send_sem,
    recv_sem,
):
    cols = elems_x * elems_y
    size_x = lax.axis_size("gx")
    size_y = lax.axis_size("gy")
    me_x = lax.axis_index("gx")
    me_y = lax.axis_index("gy")
    near_x = (lax.rem(me_x + size_x - 1, size_x), lax.rem(me_x + 1, size_x))
    near_y = (lax.rem(me_y + size_y - 1, size_y), lax.rem(me_y + 1, size_y))
    partners = [(near_x[0], me_y), (near_x[1], me_y), (me_x, near_y[0]), (me_x, near_y[1])]
    partners += [(near_x[a], near_y[b]) for a in range(2) for b in range(2)]

    barrier = pltpu.get_barrier_semaphore()
    for partner in partners:
        pl.semaphore_signal(
            barrier, inc=1, device_id=partner, device_id_type=pl.DeviceIdType.MESH
        )
    pl.semaphore_wait(barrier, len(partners))

    def copies(slot, c):
        made = []
        for d in range(8):
            if d < 2:
                src, dst = send_x.at[slot, c, d], recv_x.at[slot, c, 1 - d]
            elif d < 4:
                src, dst = send_y.at[slot, c, d - 2], recv_y.at[slot, c, 3 - d]
            else:
                src, dst = send_c.at[slot, c, d - 4], recv_c.at[slot, c, 7 - d]
            mirror = (1, 0, 3, 2, 7, 6, 5, 4)[d]
            made.append(
                pltpu.make_async_remote_copy(
                    src_ref=src,
                    dst_ref=dst,
                    send_sem=send_sem.at[slot, c, d],
                    recv_sem=recv_sem.at[slot, c, mirror],
                    device_id=partners[d],
                    device_id_type=pl.DeviceIdType.MESH,
                )
            )
        return made

    rows = lax.broadcasted_iota(jnp.int32, (N1 * cols, 128), 0) % cols
    row_x = rows % elems_x
    inner_low_y = rows >= elems_x
    inner_high_y = rows < cols - elems_x
    inner_low_x = row_x >= 1
    inner_high_x = row_x < elems_x - 1
    last_x = elems_x - 1
    last_y = cols - elems_x
    flat = (N1 * cols, 128)
    full = (N1, cols, 128)

    def local_sum(ref, c):
        zero = jnp.zeros(flat, jnp.float32)
        low = ref[c, 0].reshape(flat)
        high = ref[c, DEG].reshape(flat)
        to_low = jnp.where(inner_low_x, pltpu.roll(high, 1, 0), zero)
        to_high = jnp.where(inner_high_x, pltpu.roll(low, N1 * cols - 1, 0), zero)
        ref[c, 0] = (low + to_low).reshape(full)
        ref[c, DEG] = (high + to_high).reshape(full)
        low = ref[c, :, 0].reshape(flat)
        high = ref[c, :, DEG].reshape(flat)
        to_low = jnp.where(inner_low_y, pltpu.roll(high, elems_x, 0), zero)
        to_high = jnp.where(inner_high_y, pltpu.roll(low, N1 * cols - elems_x, 0), zero)
        ref[c, :, 0] = (low + to_low).reshape(full)
        ref[c, :, DEG] = (high + to_high).reshape(full)

    def post(ref, slot, c):
        send_y[slot, c, 0] = ref[c, :, 0, 0:elems_x, :]
        send_y[slot, c, 1] = ref[c, :, DEG, last_y:cols, :]
        for b in range(elems_y):
            at = b * elems_x
            send_x[slot, c, 0, :, b : b + 1, :] = ref[c, 0, :, at : at + 1, :]
            at = b * elems_x + last_x
            send_x[slot, c, 1, :, b : b + 1, :] = ref[c, DEG, :, at : at + 1, :]
        for a in range(2):
            for b in range(2):
                at = a * last_x + b * last_y
                send_c[slot, c, 2 * a + b] = ref[c, a * DEG, b * DEG, at : at + 1, :]
        for copy in copies(slot, c):
            copy.start()

    def collect(ref, slot, c):
        for copy in copies(slot, c):
            copy.wait()
        ref[c, :, 0, 0:elems_x, :] += recv_y[slot, c, 0]
        ref[c, :, DEG, last_y:cols, :] += recv_y[slot, c, 1]
        for b in range(elems_y):
            at = b * elems_x
            ref[c, 0, :, at : at + 1, :] += recv_x[slot, c, 0, :, b : b + 1, :]
            at = b * elems_x + last_x
            ref[c, DEG, :, at : at + 1, :] += recv_x[slot, c, 1, :, b : b + 1, :]
        for a in range(2):
            for b in range(2):
                at = a * last_x + b * last_y
                ref[c, a * DEG, b * DEG, at : at + 1, :] += recv_c[slot, c, 2 * a + b]

    nodes_x = DEG * elems_x
    nodes_y = DEG * elems_y
    nodes_z = guess_in.shape[2] // nodes_y
    pad_x = flat_a.shape[1]
    zeros_big = jnp.zeros((N1, cols, 128), jnp.float32)

    @pl.loop(0, nodes_y)
    def _(y):
        flat_a[y] = jnp.zeros((pad_x, 128), jnp.float32)
        flat_b[y] = jnp.zeros((pad_x, 128), jnp.float32)

    def through(src, dst, matrix):
        @pl.loop(0, elems_y, unroll=elems_y)
        def _(b):
            pick = pl.ds(b * DEG, DEG)
            parts = halves(src[pick].reshape(DEG * pad_x, 128))
            dst[pick] = jnp.dot(
                jnp.concatenate(parts, axis=1), matrix[...], preferred_element_type=jnp.float32
            ).reshape(DEG, pad_x, 128)

    def enter(flat_in, ref, c):
        lines = flat_in[c]
        for y in range(nodes_y):
            flat_a[y, 0:nodes_x, 0:nodes_z] = lines[:, y * nodes_z : (y + 1) * nodes_z]
        through(flat_a, flat_b, gather_in)
        ref[c, DEG] = zeros_big
        ref[c, :, DEG] = zeros_big
        for b in range(elems_y):
            for j in range(DEG):
                for i in range(DEG):
                    ref[c, i, j, b * elems_x : (b + 1) * elems_x, :] = flat_b[
                        b * DEG + j, pl.ds(i, elems_x, stride=DEG), :
                    ]

    def leave(ref, flat_out, c):
        for b in range(elems_y):
            for j in range(DEG):
                for i in range(DEG):
                    flat_b[b * DEG + j, pl.ds(i, elems_x, stride=DEG), :] = ref[
                        c, i, j, b * elems_x : (b + 1) * elems_x, :
                    ]
        through(flat_b, flat_a, select_in)
        lines = [flat_a[y, 0:nodes_x, 0:nodes_z] for y in range(nodes_y)]
        flat_out[c] = jnp.concatenate(lines, axis=1)

    @pl.loop(0, 3)
    def _(c):
        enter(guess_in, field, c)
        local_sum(field, c)
        post(field, 0, c)

    upper_edge = jnp.full((1, 128), upper[0], jnp.float32)
    lower_edge = lower_ratio[0] * upper_edge
    center = (upper_edge + lower_edge) / 2.0
    radius = (upper_edge - lower_edge) / 2.0
    sigma_ratio = center / radius
    for sweep in range(SWEEPS):
        coef[0, sweep * CHEB] = jnp.zeros((1, 128), jnp.float32)
        coef[1, sweep * CHEB] = 1.0 / center
        factor = 1.0 / sigma_ratio
        for later in range(1, CHEB):
            factor_next = 1.0 / (2.0 * sigma_ratio - factor)
            coef[0, sweep * CHEB + later] = factor_next * factor
            coef[1, sweep * CHEB + later] = 2.0 * factor_next / radius
            factor = factor_next

    kinds = jnp.concatenate([material[:, b, :] for b in range(elems_y)], axis=0)
    tables = []
    for row in range(2):
        picked = jnp.zeros(kinds.shape, jnp.float32)
        for kind in range(lame.shape[1]):
            picked = jnp.where(kinds == kind, lame[row, kind], picked)
        tables.append(
            jnp.dot(picked, spread_in[...], precision=highest, preferred_element_type=jnp.float32)
        )
    lam_all, mu_all = tables

    @pl.loop(0, N1)
    def _(i):
        for j in range(N1):
            lam_w[i, j] = lam_all * weight_in[i, j]
            mu_w[i, j] = mu_all * weight_in[i, j]

    @pl.loop(0, 3 * N1)
    def _(at):
        c = at // N1
        i = at % N1
        pieces = []
        for j in range(N1):
            own = own_in[c, i, j]
            pieces.append(lam_w[i, j] * own + mu_w[i, j] * (sum_in[i, j] + own))
        high, low = halves(jnp.concatenate(pieces, axis=0))
        summed = jnp.dot(
            jnp.concatenate([high, low], axis=1), join_in[...], preferred_element_type=jnp.float32
        )
        inverse[c, i] = summed.reshape(N1, cols, 128)

    for c in range(3):
        local_sum(inverse, c)
        post(inverse, 1, c)

    def gradients(c):
        @pl.loop(0, N1, unroll=N1)
        def _(i):
            high, low = halves(field[c, i].reshape(flat))
            both = jnp.dot(
                jnp.concatenate([high, low], axis=1),
                grad_in[...],
                preferred_element_type=jnp.float32,
            )
            for p, out in enumerate(apply_pairs(derivative, [field[c, k, i] for k in range(N1)])):
                grad_x[c, p, i] = out
            for q, out in enumerate(apply_pairs(derivative, [field[c, i, k] for k in range(N1)])):
                grad_y[c, i, q] = out
            grad_z[c, i] = (both[:, :128] + both[:, 128:]).reshape(full)

    def stresses():
        @pl.loop(0, N1, unroll=2)
        def _(i):
            for j in range(N1):
                lam = lam_w[i, j]
                mu = mu_w[i, j]
                d00, d11, d22 = grad_x[0, i, j], grad_y[1, i, j], grad_z[2, i, j]
                base = lam * (d00 + d11 + d22)
                two = mu + mu
                grad_x[0, i, j] = two * d00 + base
                grad_y[1, i, j] = two * d11 + base
                grad_z[2, i, j] = two * d22 + base
                s01 = mu * (grad_x[1, i, j] + grad_y[0, i, j])
                s02 = mu * (grad_x[2, i, j] + grad_z[0, i, j])
                s12 = mu * (grad_y[2, i, j] + grad_z[1, i, j])
                grad_x[1, i, j] = s01
                grad_y[0, i, j] = s01
                grad_x[2, i, j] = s02
                grad_z[0, i, j] = s02
                grad_y[2, i, j] = s12
                grad_z[1, i, j] = s12

    def forces(c):
        @pl.loop(0, N1, unroll=N1)
        def _(j):
            for p, out in enumerate(apply_pairs(derivative.T, [grad_x[c, k, j] for k in range(N1)])):
                resid[c, p, j] = out

        @pl.loop(0, N1, unroll=N1)
        def _(i):
            outs = apply_pairs(derivative.T, [grad_y[c, i, k] for k in range(N1)])
            inner = jnp.concatenate([resid[c, i, q] + outs[q] for q in range(N1)], axis=0)
            parts = halves(grad_z[c, i].reshape(flat)) + halves(inner)
            both = jnp.dot(
                jnp.concatenate(parts, axis=1), back_in[...], preferred_element_type=jnp.float32
            )
            resid[c, i] = source[c, i] - (both[:, :128] + both[:, 128:]).reshape(full)

    def residuals(slot):
        stresses()

        @pl.loop(0, 3)
        def _(c):
            forces(c)
            local_sum(resid, c)
            post(resid, slot, c)

    @pl.loop(0, 3)
    def _(c):
        enter(source_in, source, c)

    @pl.loop(0, 3)
    def _(c):
        collect(field, 0, c)
        gradients(c)

    @pl.loop(0, 3)
    def _(c):
        collect(inverse, 1, c)

        @pl.loop(0, N1)
        def _(i):
            inverse[c, i] = 1.0 / inverse[c, i]
            change[c, i] = zeros_big

    @pl.loop(0, steps)
    def _(step):
        slot = 2 + step % 2
        residuals(slot)

        @pl.loop(0, 3)
        def _(c):
            collect(resid, slot, c)
            alpha = coef[0, step]
            beta = coef[1, step]

            @pl.loop(0, N1, unroll=4)
            def _(i):
                new = alpha * change[c, i] + beta * (inverse[c, i] * resid[c, i])
                change[c, i] = new
                field[c, i] += new

            gradients(c)

    slot = 2 + steps % 2
    residuals(slot)

    @pl.loop(0, 3)
    def _(c):
        leave(field, smoothed_out, c)

    @pl.loop(0, 3)
    def _(c):
        collect(resid, slot, c)
        leave(resid, residual_out, c)


def z_join(blocks, clamped):
    nodes = DEG * blocks + 1
    gather = np.zeros((nodes, blocks * N1))
    for element in range(blocks):
        for k in range(N1):
            gather[DEG * element + k, element * N1 + k] = 1.0
    if clamped:
        gather[0] = 0.0
        gather[nodes - 1] = 0.0
    return gather.T @ gather


def local(right_side, guess, material, lame, upper, lower_ratio):
    elems_x, elems_y, elems_z = material.shape
    cols = elems_x * elems_y
    lanes = N1 * elems_z
    nodes_z = DEG * elems_z - 1
    weights_np, derivative_np, ratio_np = gll_tables(DEG)
    eye_z = np.eye(elems_z)
    grad_np = np.kron(eye_z, derivative_np.T)
    join_np = z_join(elems_z, True)
    back_np = np.kron(eye_z, derivative_np) @ join_np
    grad_high, grad_low = np_halves(grad_np)
    back_high, back_low = np_halves(back_np)
    none = np.zeros_like(grad_high)
    joined = join_np.astype(jnp.bfloat16)
    grad_in = jnp.asarray(np.block([[grad_high, grad_low], [grad_high, none]]))
    back_in = jnp.asarray(
        np.block([[back_high, back_low], [back_high, none], [joined, none], [joined, none]])
    )
    all_join = z_join(elems_z, False).astype(jnp.bfloat16)
    join_in = jnp.asarray(np.concatenate([all_join, all_join], axis=0))

    weights_z = np.tile(weights_np, elems_z)
    ratio_z = np.tile(ratio_np, elems_z)
    weight_np = weights_np[:, None, None] * weights_np[None, :, None] * weights_z
    shape_w = (N1, N1, lanes)
    own_x = np.broadcast_to(ratio_np[:, None, None], shape_w)
    own_y = np.broadcast_to(ratio_np[None, :, None], shape_w)
    own_z = np.broadcast_to(ratio_z, shape_w)
    own_np = np.stack([own_x, own_y, own_z])
    weight_in = jnp.asarray(weight_np[:, :, None], jnp.float32)
    own_in = jnp.asarray(own_np[:, :, :, None], jnp.float32)
    sum_in = jnp.asarray((own_x + own_y + own_z)[:, :, None], jnp.float32)

    gather_np = clamped_gather(elems_z)
    nodes_z = gather_np.shape[0]
    owned_np = gather_np.copy()
    owned_np[:, DEG::N1] = 0.0
    enter_np = np.zeros((lanes, lanes))
    enter_np[:nodes_z] = gather_np
    leave_np = np.zeros((lanes, lanes))
    leave_np[:, :nodes_z] = owned_np.T
    gather_in = jnp.asarray(np.concatenate([enter_np, enter_np], axis=0).astype(jnp.bfloat16))
    select_in = jnp.asarray(np.concatenate([leave_np, leave_np], axis=0).astype(jnp.bfloat16))
    spread_in = jnp.asarray(np.kron(eye_z, np.ones((1, N1))), dtype=jnp.float32)

    pad_x = -(-DEG * elems_x // 8) * 8
    whole = (3, N1, N1, cols, lanes)
    vmem = pl.BlockSpec(memory_space=pltpu.VMEM)
    smem = pl.BlockSpec(memory_space=pltpu.SMEM)
    big = pltpu.VMEM(whole, jnp.float32)
    small = pltpu.VMEM((N1, N1, cols, lanes), jnp.float32)
    lines = pltpu.VMEM((DEG * elems_y, pad_x, lanes), jnp.float32)
    face_x = pltpu.VMEM((SLOTS, 3, 2, N1, elems_y, lanes), jnp.float32)
    face_y = pltpu.VMEM((SLOTS, 3, 2, N1, elems_x, lanes), jnp.float32)
    corner = pltpu.VMEM((SLOTS, 3, 4, 1, lanes), jnp.float32)
    shape = jax.ShapeDtypeStruct(guess.shape, jnp.float32)

    def kernel(*refs):
        smoother_kernel(SWEEPS * CHEB, elems_x, elems_y, derivative_np, *refs)

    return pl.pallas_call(
        kernel,
        out_shape=(shape, shape),
        in_specs=[smem] * 3 + [vmem] * 12,
        out_specs=(vmem, vmem),
        scratch_shapes=[pltpu.VMEM((2, SWEEPS * CHEB, 1, lanes), jnp.float32)]
        + [big] * 3
        + [small] * 2
        + [big] * 5
        + [lines] * 2
        + [face_x, face_y, corner] * 2
        + [pltpu.SemaphoreType.DMA((SLOTS, 3, 8))] * 2,
        compiler_params=pltpu.CompilerParams(collective_id=0, has_side_effects=True),
    )(
        lame,
        upper,
        lower_ratio,
        guess,
        right_side,
        material,
        weight_in,
        own_in,
        sum_in,
        spread_in,
        gather_in,
        select_in,
        grad_in,
        back_in,
        join_in,
    )


def solution(mesh):
    placed = (P(None, "gx", "gy"), P(None, "gx", "gy"), P("gx", "gy", None), P(), P(), P())
    return jax.shard_map(
        local,
        mesh=mesh,
        in_specs=placed,
        out_specs=(P(None, "gx", "gy"), P(None, "gx", "gy")),
        check_vma=False,
    )
```

```python
import jax
import jax.numpy as jnp
import numpy as np
from jax import lax
from jax.experimental import pallas as pl
from jax.experimental.pallas import tpu as pltpu
from jax.sharding import PartitionSpec as P

DEG = 7
SWEEPS = 2
CHEB = 3


highest = lax.Precision.HIGHEST


def legendre_pair(points, degree):
    prev_poly = points * 0.0 + 1.0
    this_poly = points * 1.0
    for order in range(2, degree + 1):
        next_poly = ((2 * order - 1) * points * this_poly - (order - 1) * prev_poly) / order
        prev_poly = this_poly
        this_poly = next_poly
    return (this_poly, prev_poly)


def gll_tables(degree):
    count = degree + 1
    points = -np.cos(np.pi * np.arange(count) / degree)
    for newton_step in range(60):
        this_poly, prev_poly = legendre_pair(points, degree)
        points = points - (points * this_poly - prev_poly) / (count * this_poly)
    values, unused_poly = legendre_pair(points, degree)
    weights = 2.0 / (degree * (degree + 1) * values**2)
    identity_np = np.eye(count)
    spacing = points[:, None] - points[None, :] + identity_np
    derivative = values[:, None] / (values[None, :] * spacing) * (1.0 - identity_np)
    derivative[0, 0] = -degree * (degree + 1) / 4.0
    derivative[degree, degree] = degree * (degree + 1) / 4.0
    stiff_ratio = (weights[:, None] * derivative**2).sum(0) / weights
    return (weights, derivative, stiff_ratio)


def clamped_gather(blocks):
    free_nodes = DEG * blocks - 1
    selector = np.zeros((free_nodes, blocks * (DEG + 1)), np.float32)
    for element in range(blocks):
        for node_idx in range(DEG + 1):
            target = DEG * element + node_idx - 1
            if 0 <= target < free_nodes:
                selector[target, element * (DEG + 1) + node_idx] = 1.0
    return selector


N1 = DEG + 1
SLOTS = 4


def halves(value):
    high = value.astype(jnp.bfloat16)
    low = (value - high.astype(jnp.float32)).astype(jnp.bfloat16)
    return high, low


def np_halves(matrix):
    high = np.asarray(matrix, np.float32).astype(jnp.bfloat16)
    low = (np.asarray(matrix, np.float64) - high.astype(np.float64)).astype(jnp.bfloat16)
    return high, low


def apply_pairs(matrix, values):
    half = N1 // 2
    even = [values[i] + values[DEG - i] for i in range(half)]
    odd = [values[i] - values[DEG - i] for i in range(half)]
    outs = [None] * N1
    for p in range(half):
        plus = None
        minus = None
        for i in range(half):
            by_even = float(np.float32((matrix[p, i] + matrix[p, DEG - i]) / 2))
            by_odd = float(np.float32((matrix[p, i] - matrix[p, DEG - i]) / 2))
            plus = by_even * even[i] if plus is None else plus + by_even * even[i]
            minus = by_odd * odd[i] if minus is None else minus + by_odd * odd[i]
        outs[p] = minus + plus
        outs[DEG - p] = minus - plus
    return outs


def smoother_kernel(
    steps,
    elems_x,
    elems_y,
    derivative,
    lame,
    upper,
    lower_ratio,
    guess_in,
    source_in,
    material,
    weight_in,
    own_in,
    sum_in,
    spread_in,
    gather_in,
    select_in,
    grad_in,
    back_in,
    join_in,
    smoothed_out,
    residual_out,
    coef,
    field,
    resid,
    source,
    lam_w,
    mu_w,
    inverse,
    change,
    grad_x,
    grad_y,
    grad_z,
    flat_a,
    flat_b,
    send_x,
    send_y,
    send_c,
    recv_x,
    recv_y,
    recv_c,
    send_sem,
    recv_sem,
):
    cols = elems_x * elems_y
    size_x = lax.axis_size("gx")
    size_y = lax.axis_size("gy")
    me_x = lax.axis_index("gx")
    me_y = lax.axis_index("gy")
    near_x = (lax.rem(me_x + size_x - 1, size_x), lax.rem(me_x + 1, size_x))
    near_y = (lax.rem(me_y + size_y - 1, size_y), lax.rem(me_y + 1, size_y))
    partners = [(near_x[0], me_y), (near_x[1], me_y), (me_x, near_y[0]), (me_x, near_y[1])]
    partners += [(near_x[a], near_y[b]) for a in range(2) for b in range(2)]

    barrier = pltpu.get_barrier_semaphore()
    for partner in partners:
        pl.semaphore_signal(
            barrier, inc=1, device_id=partner, device_id_type=pl.DeviceIdType.MESH
        )
    pl.semaphore_wait(barrier, len(partners))

    def copies(slot, c):
        made = []
        for d in range(8):
            if d < 2:
                src, dst = send_x.at[slot, c, d], recv_x.at[slot, c, 1 - d]
            elif d < 4:
                src, dst = send_y.at[slot, c, d - 2], recv_y.at[slot, c, 3 - d]
            else:
                src, dst = send_c.at[slot, c, d - 4], recv_c.at[slot, c, 7 - d]
            mirror = (1, 0, 3, 2, 7, 6, 5, 4)[d]
            made.append(
                pltpu.make_async_remote_copy(
                    src_ref=src,
                    dst_ref=dst,
                    send_sem=send_sem.at[slot, c, d],
                    recv_sem=recv_sem.at[slot, c, mirror],
                    device_id=partners[d],
                    device_id_type=pl.DeviceIdType.MESH,
                )
            )
        return made

    rows = lax.broadcasted_iota(jnp.int32, (N1 * cols, 128), 0) % cols
    row_x = rows % elems_x
    inner_low_y = rows >= elems_x
    inner_high_y = rows < cols - elems_x
    inner_low_x = row_x >= 1
    inner_high_x = row_x < elems_x - 1
    last_x = elems_x - 1
    last_y = cols - elems_x
    flat = (N1 * cols, 128)
    full = (N1, cols, 128)

    def local_sum(ref, c):
        zero = jnp.zeros(flat, jnp.float32)
        low = ref[c, 0].reshape(flat)
        high = ref[c, DEG].reshape(flat)
        to_low = jnp.where(inner_low_x, pltpu.roll(high, 1, 0), zero)
        to_high = jnp.where(inner_high_x, pltpu.roll(low, N1 * cols - 1, 0), zero)
        ref[c, 0] = (low + to_low).reshape(full)
        ref[c, DEG] = (high + to_high).reshape(full)
        low = ref[c, :, 0].reshape(flat)
        high = ref[c, :, DEG].reshape(flat)
        to_low = jnp.where(inner_low_y, pltpu.roll(high, elems_x, 0), zero)
        to_high = jnp.where(inner_high_y, pltpu.roll(low, N1 * cols - elems_x, 0), zero)
        ref[c, :, 0] = (low + to_low).reshape(full)
        ref[c, :, DEG] = (high + to_high).reshape(full)

    def post(ref, slot, c):
        send_y[slot, c, 0] = ref[c, :, 0, 0:elems_x, :]
        send_y[slot, c, 1] = ref[c, :, DEG, last_y:cols, :]
        for b in range(elems_y):
            at = b * elems_x
            send_x[slot, c, 0, :, b : b + 1, :] = ref[c, 0, :, at : at + 1, :]
            at = b * elems_x + last_x
            send_x[slot, c, 1, :, b : b + 1, :] = ref[c, DEG, :, at : at + 1, :]
        for a in range(2):
            for b in range(2):
                at = a * last_x + b * last_y
                send_c[slot, c, 2 * a + b] = ref[c, a * DEG, b * DEG, at : at + 1, :]
        for copy in copies(slot, c):
            copy.start()

    def collect(ref, slot, c):
        for copy in copies(slot, c):
            copy.wait()
        ref[c, :, 0, 0:elems_x, :] += recv_y[slot, c, 0]
        ref[c, :, DEG, last_y:cols, :] += recv_y[slot, c, 1]
        for b in range(elems_y):
            at = b * elems_x
            ref[c, 0, :, at : at + 1, :] += recv_x[slot, c, 0, :, b : b + 1, :]
            at = b * elems_x + last_x
            ref[c, DEG, :, at : at + 1, :] += recv_x[slot, c, 1, :, b : b + 1, :]
        for a in range(2):
            for b in range(2):
                at = a * last_x + b * last_y
                ref[c, a * DEG, b * DEG, at : at + 1, :] += recv_c[slot, c, 2 * a + b]

    nodes_x = DEG * elems_x
    nodes_y = DEG * elems_y
    nodes_z = guess_in.shape[2] // nodes_y
    pad_x = flat_a.shape[1]
    zeros_big = jnp.zeros((N1, cols, 128), jnp.float32)

    @pl.loop(0, nodes_y)
    def _(y):
        flat_a[y] = jnp.zeros((pad_x, 128), jnp.float32)
        flat_b[y] = jnp.zeros((pad_x, 128), jnp.float32)

    def through(src, dst, matrix):
        @pl.loop(0, elems_y, unroll=elems_y)
        def _(b):
            pick = pl.ds(b * DEG, DEG)
            parts = halves(src[pick].reshape(DEG * pad_x, 128))
            dst[pick] = jnp.dot(
                jnp.concatenate(parts, axis=1), matrix[...], preferred_element_type=jnp.float32
            ).reshape(DEG, pad_x, 128)

    def enter(flat_in, ref, c):
        lines = flat_in[c]
        for y in range(nodes_y):
            flat_a[y, 0:nodes_x, 0:nodes_z] = lines[:, y * nodes_z : (y + 1) * nodes_z]
        through(flat_a, flat_b, gather_in)
        ref[c, DEG] = zeros_big
        ref[c, :, DEG] = zeros_big
        for b in range(elems_y):
            for j in range(DEG):
                for i in range(DEG):
                    ref[c, i, j, b * elems_x : (b + 1) * elems_x, :] = flat_b[
                        b * DEG + j, pl.ds(i, elems_x, stride=DEG), :
                    ]

    def leave(ref, flat_out, c):
        for b in range(elems_y):
            for j in range(DEG):
                for i in range(DEG):
                    flat_b[b * DEG + j, pl.ds(i, elems_x, stride=DEG), :] = ref[
                        c, i, j, b * elems_x : (b + 1) * elems_x, :
                    ]
        through(flat_b, flat_a, select_in)
        lines = [flat_a[y, 0:nodes_x, 0:nodes_z] for y in range(nodes_y)]
        flat_out[c] = jnp.concatenate(lines, axis=1)

    @pl.loop(0, 3)
    def _(c):
        enter(guess_in, field, c)
        local_sum(field, c)
        post(field, 0, c)

    upper_edge = jnp.full((1, 128), upper[0], jnp.float32)
    lower_edge = lower_ratio[0] * upper_edge
    center = (upper_edge + lower_edge) / 2.0
    radius = (upper_edge - lower_edge) / 2.0
    sigma_ratio = center / radius
    for sweep in range(SWEEPS):
        coef[0, sweep * CHEB] = jnp.zeros((1, 128), jnp.float32)
        coef[1, sweep * CHEB] = 1.0 / center
        factor = 1.0 / sigma_ratio
        for later in range(1, CHEB):
            factor_next = 1.0 / (2.0 * sigma_ratio - factor)
            coef[0, sweep * CHEB + later] = factor_next * factor
            coef[1, sweep * CHEB + later] = 2.0 * factor_next / radius
            factor = factor_next

    kinds = jnp.concatenate([material[:, b, :] for b in range(elems_y)], axis=0)
    tables = []
    for row in range(2):
        picked = jnp.zeros(kinds.shape, jnp.float32)
        for kind in range(lame.shape[1]):
            picked = jnp.where(kinds == kind, lame[row, kind], picked)
        tables.append(
            jnp.dot(picked, spread_in[...], precision=highest, preferred_element_type=jnp.float32)
        )
    lam_all, mu_all = tables

    @pl.loop(0, N1)
    def _(i):
        for j in range(N1):
            lam_w[i, j] = lam_all * weight_in[i, j]
            mu_w[i, j] = mu_all * weight_in[i, j]

    @pl.loop(0, 3 * N1, unroll=N1)
    def _(at):
        c = at // N1
        i = at % N1
        pieces = []
        for j in range(N1):
            own = own_in[c, i, j]
            pieces.append(lam_w[i, j] * own + mu_w[i, j] * (sum_in[i, j] + own))
        high, low = halves(jnp.concatenate(pieces, axis=0))
        summed = jnp.dot(
            jnp.concatenate([high, low], axis=1), join_in[...], preferred_element_type=jnp.float32
        )
        inverse[c, i] = summed.reshape(N1, cols, 128)

    for c in range(3):
        local_sum(inverse, c)
        post(inverse, 1, c)

    def gradients(c):
        @pl.loop(0, N1, unroll=N1)
        def _(i):
            high, low = halves(field[c, i].reshape(flat))
            both = jnp.dot(
                jnp.concatenate([high, low], axis=1),
                grad_in[...],
                preferred_element_type=jnp.float32,
            )
            for p, out in enumerate(apply_pairs(derivative, [field[c, k, i] for k in range(N1)])):
                grad_x[c, p, i] = out
            for q, out in enumerate(apply_pairs(derivative, [field[c, i, k] for k in range(N1)])):
                grad_y[c, i, q] = out
            grad_z[c, i] = (both[:, :128] + both[:, 128:]).reshape(full)

    def stresses():
        @pl.loop(0, N1, unroll=N1)
        def _(i):
            for j in range(N1):
                lam = lam_w[i, j]
                mu = mu_w[i, j]
                d00, d11, d22 = grad_x[0, i, j], grad_y[1, i, j], grad_z[2, i, j]
                base = lam * (d00 + d11 + d22)
                two = mu + mu
                grad_x[0, i, j] = two * d00 + base
                grad_y[1, i, j] = two * d11 + base
                grad_z[2, i, j] = two * d22 + base
                s01 = mu * (grad_x[1, i, j] + grad_y[0, i, j])
                s02 = mu * (grad_x[2, i, j] + grad_z[0, i, j])
                s12 = mu * (grad_y[2, i, j] + grad_z[1, i, j])
                grad_x[1, i, j] = s01
                grad_y[0, i, j] = s01
                grad_x[2, i, j] = s02
                grad_z[0, i, j] = s02
                grad_y[2, i, j] = s12
                grad_z[1, i, j] = s12

    def forces(c):
        @pl.loop(0, N1, unroll=N1)
        def _(j):
            for p, out in enumerate(apply_pairs(derivative.T, [grad_x[c, k, j] for k in range(N1)])):
                resid[c, p, j] = out

        @pl.loop(0, N1, unroll=N1)
        def _(i):
            outs = apply_pairs(derivative.T, [grad_y[c, i, k] for k in range(N1)])
            inner = jnp.concatenate([resid[c, i, q] + outs[q] for q in range(N1)], axis=0)
            parts = halves(grad_z[c, i].reshape(flat)) + halves(inner)
            both = jnp.dot(
                jnp.concatenate(parts, axis=1), back_in[...], preferred_element_type=jnp.float32
            )
            resid[c, i] = source[c, i] - (both[:, :128] + both[:, 128:]).reshape(full)

    def residuals(slot):
        stresses()

        @pl.loop(0, 3)
        def _(c):
            forces(c)
            local_sum(resid, c)
            post(resid, slot, c)

    @pl.loop(0, 3)
    def _(c):
        enter(source_in, source, c)

    @pl.loop(0, 3)
    def _(c):
        collect(field, 0, c)
        gradients(c)

    @pl.loop(0, 3)
    def _(c):
        collect(inverse, 1, c)

        @pl.loop(0, N1)
        def _(i):
            inverse[c, i] = 1.0 / inverse[c, i]
            change[c, i] = zeros_big

    @pl.loop(0, steps)
    def _(step):
        slot = 2 + step % 2
        residuals(slot)

        @pl.loop(0, 3)
        def _(c):
            collect(resid, slot, c)
            alpha = coef[0, step]
            beta = coef[1, step]

            @pl.loop(0, N1, unroll=N1)
            def _(i):
                new = alpha * change[c, i] + beta * (inverse[c, i] * resid[c, i])
                change[c, i] = new
                field[c, i] += new

            gradients(c)

    slot = 2 + steps % 2
    residuals(slot)

    @pl.loop(0, 3)
    def _(c):
        leave(field, smoothed_out, c)

    @pl.loop(0, 3)
    def _(c):
        collect(resid, slot, c)
        leave(resid, residual_out, c)


def z_join(blocks, clamped):
    nodes = DEG * blocks + 1
    gather = np.zeros((nodes, blocks * N1))
    for element in range(blocks):
        for k in range(N1):
            gather[DEG * element + k, element * N1 + k] = 1.0
    if clamped:
        gather[0] = 0.0
        gather[nodes - 1] = 0.0
    return gather.T @ gather


def local(right_side, guess, material, lame, upper, lower_ratio):
    elems_x, elems_y, elems_z = material.shape
    cols = elems_x * elems_y
    lanes = N1 * elems_z
    nodes_z = DEG * elems_z - 1
    weights_np, derivative_np, ratio_np = gll_tables(DEG)
    eye_z = np.eye(elems_z)
    grad_np = np.kron(eye_z, derivative_np.T)
    join_np = z_join(elems_z, True)
    back_np = np.kron(eye_z, derivative_np) @ join_np
    grad_high, grad_low = np_halves(grad_np)
    back_high, back_low = np_halves(back_np)
    none = np.zeros_like(grad_high)
    joined = join_np.astype(jnp.bfloat16)
    grad_in = jnp.asarray(np.block([[grad_high, grad_low], [grad_high, none]]))
    back_in = jnp.asarray(
        np.block([[back_high, back_low], [back_high, none], [joined, none], [joined, none]])
    )
    all_join = z_join(elems_z, False).astype(jnp.bfloat16)
    join_in = jnp.asarray(np.concatenate([all_join, all_join], axis=0))

    weights_z = np.tile(weights_np, elems_z)
    ratio_z = np.tile(ratio_np, elems_z)
    weight_np = weights_np[:, None, None] * weights_np[None, :, None] * weights_z
    shape_w = (N1, N1, lanes)
    own_x = np.broadcast_to(ratio_np[:, None, None], shape_w)
    own_y = np.broadcast_to(ratio_np[None, :, None], shape_w)
    own_z = np.broadcast_to(ratio_z, shape_w)
    own_np = np.stack([own_x, own_y, own_z])
    weight_in = jnp.asarray(weight_np[:, :, None], jnp.float32)
    own_in = jnp.asarray(own_np[:, :, :, None], jnp.float32)
    sum_in = jnp.asarray((own_x + own_y + own_z)[:, :, None], jnp.float32)

    gather_np = clamped_gather(elems_z)
    nodes_z = gather_np.shape[0]
    owned_np = gather_np.copy()
    owned_np[:, DEG::N1] = 0.0
    enter_np = np.zeros((lanes, lanes))
    enter_np[:nodes_z] = gather_np
    leave_np = np.zeros((lanes, lanes))
    leave_np[:, :nodes_z] = owned_np.T
    gather_in = jnp.asarray(np.concatenate([enter_np, enter_np], axis=0).astype(jnp.bfloat16))
    select_in = jnp.asarray(np.concatenate([leave_np, leave_np], axis=0).astype(jnp.bfloat16))
    spread_in = jnp.asarray(np.kron(eye_z, np.ones((1, N1))), dtype=jnp.float32)

    pad_x = -(-DEG * elems_x // 8) * 8
    whole = (3, N1, N1, cols, lanes)
    vmem = pl.BlockSpec(memory_space=pltpu.VMEM)
    smem = pl.BlockSpec(memory_space=pltpu.SMEM)
    big = pltpu.VMEM(whole, jnp.float32)
    small = pltpu.VMEM((N1, N1, cols, lanes), jnp.float32)
    lines = pltpu.VMEM((DEG * elems_y, pad_x, lanes), jnp.float32)
    face_x = pltpu.VMEM((SLOTS, 3, 2, N1, elems_y, lanes), jnp.float32)
    face_y = pltpu.VMEM((SLOTS, 3, 2, N1, elems_x, lanes), jnp.float32)
    corner = pltpu.VMEM((SLOTS, 3, 4, 1, lanes), jnp.float32)
    shape = jax.ShapeDtypeStruct(guess.shape, jnp.float32)

    def kernel(*refs):
        smoother_kernel(SWEEPS * CHEB, elems_x, elems_y, derivative_np, *refs)

    return pl.pallas_call(
        kernel,
        out_shape=(shape, shape),
        in_specs=[smem] * 3 + [vmem] * 12,
        out_specs=(vmem, vmem),
        scratch_shapes=[pltpu.VMEM((2, SWEEPS * CHEB, 1, lanes), jnp.float32)]
        + [big] * 3
        + [small] * 2
        + [big] * 5
        + [lines] * 2
        + [face_x, face_y, corner] * 2
        + [pltpu.SemaphoreType.DMA((SLOTS, 3, 8))] * 2,
        compiler_params=pltpu.CompilerParams(collective_id=0, has_side_effects=True),
    )(
        lame,
        upper,
        lower_ratio,
        guess,
        right_side,
        material,
        weight_in,
        own_in,
        sum_in,
        spread_in,
        gather_in,
        select_in,
        grad_in,
        back_in,
        join_in,
    )


def solution(mesh):
    placed = (P(None, "gx", "gy"), P(None, "gx", "gy"), P("gx", "gy", None), P(), P(), P())
    return jax.shard_map(
        local,
        mesh=mesh,
        in_specs=placed,
        out_specs=(P(None, "gx", "gy"), P(None, "gx", "gy")),
        check_vma=False,
    )
```
